32 devices in a mesh: row: 8 (over z, core), col: 4 (over y, x).
Axes of the slice: x: 2, y: 2, z: 4, core: 2. Of those that a mesh axis runs over, the one named last changes fastest.
Arguments:
- train_weight: bfloat16 [4, 4608, 2048], P(None, 'row', 'col')
- src_map: int32 [16], replicated, may hold values from 0 to 15, as said below
- tgt_map: int32 [16], replicated, may hold values from 0 to 15, as said below
- probe: bfloat16 [4096, 4608], P('row'), may hold values from -6 to 6
Outputs:
- codes: bfloat16 [4, 4608, 2048], P(None, None, 'col')
- peaks: float32 [4, 16], P(None, 'col')
- checked: bfloat16 [4, 4096, 2048], P(None, 'row', 'col')
The draws below stay inside these ranges and needn't reach their ends.
Inputs may be any that keep to these rules, and one draw needn't show every extreme that they name: src_map is a permutation of 0 to 15. tgt_map is a permutation of 0 to 15. Call column k the slots k * 4 to (k + 1) * 4 - 1 of a map, and let C = 4. There are three different offsets a, b, c in 0 to C - 1, the same for every column, of which one is C / 2 and one is C - 1: the heads of training column k stand in serving columns (k - a) mod C (2 of them), (k - b) mod C (one) and (k - c) mod C (one).
All inputs are finite; a program needn't handle non-finite values. Where the reference program divides by a largest or mean magnitude, that divisor is 1e-20 or more.
Results may differ from the reference program's by a relative error of at most 0.0049.
Values may be sent and summed in bfloat16 or wider, within the bound.
A program may use at most 128 MiB of HBM per device.

```python
import jax
import jax.numpy as jnp

D = 4608
HDIM = 128
HCOL = 4
LAYERS = 4
TOKENS = 4096
N_COL = 4


def head_maps(key):
    heads_all = HCOL * N_COL
    keys = jax.random.split(jax.random.fold_in(key, 17), 6)
    source = jax.random.permutation(keys[0], heads_all).astype(jnp.int32)
    half = N_COL // 2
    before_one = jnp.array([N_COL - 1], jnp.int32)
    picked = jax.random.randint(keys[5], (1,), 0, N_COL - 2).astype(jnp.int32)
    third = jnp.where(picked < half, picked, picked + 1).astype(jnp.int32)
    three = jnp.concatenate([jnp.array([half], jnp.int32), before_one, third])
    offsets = three[jax.random.permutation(keys[4], 3)].astype(jnp.int32)
    pattern = jnp.array([0, 0, 1, 2], jnp.int32)
    roles = jax.vmap(lambda single: jax.random.permutation(single, 4))(jax.random.split(keys[2], N_COL)).astype(jnp.int32)
    locals_order = jax.vmap(lambda single: jax.random.permutation(single, 4))(jax.random.split(keys[3], N_COL)).astype(jnp.int32)
    targets = jnp.arange(N_COL, dtype=jnp.int32)[:, None]
    shifted = offsets[pattern[roles]]
    from_col = (targets + shifted) % N_COL
    local_slot = locals_order[from_col, roles]
    target = source[(from_col * HCOL + local_slot).reshape(-1)]
    return (source, target.astype(jnp.int32))


def draw_src_map(key, part):
    return head_maps(key)[0]


def draw_tgt_map(key, part):
    return head_maps(key)[1]


def draw_train_weight(key, part):
    keys = jax.random.split(jax.random.fold_in(key, 5), 3)
    heads_all = HCOL * N_COL
    head_scale = jnp.exp(jax.random.uniform(keys[1], (LAYERS, 1, heads_all, 1), jnp.float32, jnp.log(0.3), jnp.log(3.0)))
    row_scale = jnp.exp(jax.random.uniform(keys[2], (1, D, 1, 1), jnp.float32, jnp.log(0.4), jnp.log(4.0)))
    base = jax.random.normal(keys[0], (LAYERS, D, heads_all, HDIM), jnp.float32)
    weights = base * head_scale * row_scale / jnp.sqrt(jnp.float32(D))
    return weights.reshape(LAYERS, D, heads_all * HDIM).astype(jnp.bfloat16)


def block_scale(stream_key, shape, cuts, smallest, high):
    def one(position, shards_of):
        heights = jax.random.uniform(jax.random.fold_in(jax.random.fold_in(stream_key, 6), position), (shards_of,), jnp.float32, smallest / len(cuts), high / len(cuts))
        return jnp.repeat(jnp.exp(heights), shape[position] // shards_of).reshape((-1,) + (1,) * (len(shape) - position - 1))

    loudness = one(*cuts[0])
    for cut in cuts[1:]:
        loudness = loudness * one(*cut)
    return loudness


def bell_draw(stream_key, shape, spread, most, cuts=(), kind=jnp.bfloat16):
    loudness = block_scale(stream_key, shape, cuts, -0.22, 0.18) if cuts else 1.0
    entries = jax.random.normal(stream_key, shape, jnp.float32) * spread * loudness
    return jnp.minimum(jnp.maximum(entries, -most), most).astype(kind)


def setup_inputs(seed: int = 0) -> dict:
    streams_of = jax.random.split(jax.random.key(seed), 5)
    return {
        "train_weight": draw_train_weight(jax.random.fold_in(streams_of[4], 71), 0),
        "src_map": draw_src_map(jax.random.fold_in(streams_of[4], 71), 0),
        "tgt_map": draw_tgt_map(jax.random.fold_in(streams_of[4], 71), 0),
        "probe": bell_draw(streams_of[3], (TOKENS, D), 1.0, 6.0, ((0, 8),)),
    }


def reference(train_weight, src_map, tgt_map, probe):
    heads_all = src_map.shape[0]
    slot_ids = jnp.arange(heads_all, dtype=jnp.int32)
    matched = (src_map[None, :] == tgt_map[:, None]).astype(jnp.int32)
    source = jnp.sum(matched * slot_ids[None, :], axis=1).astype(jnp.int32)
    heads_four = train_weight.reshape(LAYERS, D, heads_all, HDIM)
    served = jnp.take(heads_four, source, axis=2)
    peaks = jnp.max(jnp.abs(served.astype(jnp.float32)), axis=(1, 3))
    codes = (served.astype(jnp.float32) / (peaks[:, None, :, None] + 1e-6)).astype(jnp.bfloat16)
    codes = codes.reshape(LAYERS, D, heads_all * HDIM)
    results = []
    for layer in range(LAYERS):
        projected = jnp.dot(probe, codes[layer], preferred_element_type=jnp.float32)
        scaled = projected * jnp.repeat(peaks[layer], HDIM)[None, :]
        results.append(scaled.astype(jnp.bfloat16))
    return codes, peaks, jnp.stack(results)
```

```python
import functools

import jax
import jax.numpy as jnp
from jax import lax
from jax.experimental import pallas as pl
from jax.experimental.pallas import tpu as pltpu
from jax.sharding import PartitionSpec as P

HDIM = 128
CORES = 2
TILE = 16
KSTEP = 512
SLOTS = 2
MESH = pl.DeviceIdType.MESH


def split(rows, shares):
    units, total = rows // TILE, sum(shares)
    cuts = [units * sum(shares[:i]) // total for i in range(len(shares) + 1)]
    return [(a * TILE, (b - a) * TILE) for a, b in zip(cuts, cuts[1:]) if b > a]


def piece_list(layers, rows):
    out = []
    for layer in range(layers):
        shares = (1, 2, 3, 6) if layer == 0 else ((3, 2, 1) if layer == layers - 1 else (1, 1))
        out.extend((layer, r0, size) for r0, size in split(rows, shares))
    return out


def tops_of(read, width, pair):
    def most(i, acc):
        at = pl.ds(pl.multiple_of(i * KSTEP, KSTEP), KSTEP)
        return tuple(
            jnp.maximum(a, jnp.max(jnp.abs(read(t, at)).reshape(-1, TILE, HDIM), axis=0))
            for a, t in zip(acc, pair)
        )

    zero = jnp.zeros((TILE, HDIM), jnp.bfloat16)
    best = lax.fori_loop(0, width // KSTEP, most, (zero,) * len(pair))
    return [
        jnp.max(jnp.max(b.astype(jnp.float32), axis=0, keepdims=True), axis=1, keepdims=True)
        for b in best
    ]


def project(read, write, pbuf, tops, width, pair):
    spread = [jnp.broadcast_to(p, (1, HDIM)) for p in tops]
    inverse = [1.0 / ((p + 1e-06) * 0.25) for p in spread]

    def step(i, acc):
        at = pl.ds(pl.multiple_of(i * KSTEP, KSTEP), KSTEP)
        both = jnp.concatenate(
            [
                ((read(t, at).astype(jnp.float32) * 0.25) * inv).astype(jnp.bfloat16)
                for t, inv in zip(pair, inverse)
            ],
            axis=1,
        )
        write(i, at, both)
        return acc + jnp.dot(pbuf[:, at], both, preferred_element_type=jnp.float32)

    zero = jnp.zeros((pbuf.shape[0], len(pair) * HDIM), jnp.float32)
    acc = lax.fori_loop(0, width // KSTEP, step, zero)
    return acc * jnp.concatenate(spread, axis=1)


def note_tops(peaks_ref, layer, pair, tops):
    here = lax.broadcasted_iota(jnp.int32, peaks_ref.shape, 0) == layer
    lane = lax.broadcasted_iota(jnp.int32, peaks_ref.shape, 1)
    for t, top in zip(pair, tops):
        peaks_ref[...] = jnp.where(here & (lane == t), top, peaks_ref[...])


def gather_kernel(
    pieces, zs, cols, src_map, tgt_map, w_ref, probe_ref,
    checked_ref, last_ref, pbuf, peaks_ref, *refs,
):
    layers, rows, _ = w_ref.shape
    codes_refs, refs = refs[: layers - 1], refs[layers - 1 :]
    (
        full, pack, zown, zpack, zland, guard, table,
        local, probesem, csend, crecv, zsend, zrecv,
        rawsend, rawrecv, rsend, rrecv, psend, precv, *bufs,
    ) = refs
    count = len(pieces)
    own, land = bufs[:count], bufs[count:]
    heads, width, _ = last_ref.shape
    me = lax.axis_index("row")
    mycol = lax.axis_index("col")
    z = me // CORES
    core = me % CORES
    partner = z * CORES + (1 - core)
    down, up = me - CORES, me + CORES
    has_down, has_up = z > 0, z < zs - 1
    low, high = z == 0, z == zs - 1
    is_end = low | high
    near = jnp.where(low, 1, zs - 2)
    first = [g for g in range(count) if pieces[g][0] == 0]

    def layer_ref(layer):
        return last_ref if layer == layers - 1 else full.at[layer]

    def own_copy(g, head):
        layer, r0, size = pieces[g]
        return pltpu.make_async_copy(
            w_ref.at[layer, pl.ds(r0, size), pl.ds(head * HDIM, HDIM)],
            own[g].at[head],
            local.at[g, head],
        )

    def target_of(o):
        return lax.rem(mycol + cols - o, cols)

    barrier = pltpu.get_barrier_semaphore()
    for o in range(1, cols):
        pl.semaphore_signal(barrier, inc=1, device_id={"col": target_of(o)}, device_id_type=MESH)
    pl.semaphore_signal(barrier, inc=1, device_id={"row": partner}, device_id_type=MESH)

    @pl.when(has_down)
    def _():
        pl.semaphore_signal(barrier, inc=1, device_id={"row": down}, device_id_type=MESH)

    @pl.when(has_up)
    def _():
        pl.semaphore_signal(barrier, inc=1, device_id={"row": up}, device_id_type=MESH)

    for g in range(count):
        for head in range(heads):
            own_copy(g, head).start()
    probe_copy = pltpu.make_async_copy(probe_ref, pbuf, probesem.at[0])
    probe_copy.start()
    peaks_ref[...] = jnp.zeros_like(peaks_ref)

    total = cols * heads
    mine = [src_map[mycol * heads + s] for s in range(heads)]
    want = [tgt_map[mycol * heads + t] for t in range(heads)]
    goes = [jnp.int32(0)] * heads
    for p in range(heads, total):
        wanted = tgt_map[p]
        goes = [g + jnp.where(m == wanted, p // heads, 0) for g, m in zip(goes, mine)]
    for o in range(cols):
        to = target_of(o)
        seen, picks = jnp.int32(0), [jnp.int32(0)] * SLOTS
        for s in range(heads):
            hit = goes[s] == to
            picks = [jnp.where(hit & (seen == j), s, q) for j, q in enumerate(picks)]
            seen = seen + jnp.where(hit, 1, 0)
        for j in range(SLOTS):
            table[o * SLOTS + j] = picks[j]
    slot_of = [jnp.int32(0)] * heads
    for c in range(cols):
        seen = jnp.int32(0)
        for s in range(heads):
            held = src_map[c * heads + s]
            for t in range(heads):
                slot_of[t] = jnp.where(want[t] == held, c * SLOTS + seen, slot_of[t])
            hit = want[0] == held
            for t in range(1, heads):
                hit = hit | (want[t] == held)
            seen = jnp.minimum(seen + jnp.where(hit, 1, 0), SLOTS - 1)
    for t in range(heads):
        table[cols * SLOTS + t] = slot_of[t]

    pl.semaphore_wait(barrier, cols + has_down.astype(jnp.int32) + has_up.astype(jnp.int32))

    def raw_copy(g, way, target):
        _, r0, size = pieces[g]
        return pltpu.make_async_remote_copy(
            src_ref=own[g],
            dst_ref=zown.at[:, pl.ds(r0, size), :],
            send_sem=rawsend.at[g, way],
            recv_sem=rawrecv.at[g],
            device_id={"row": target},
            device_id_type=MESH,
        )

    def col_copy(g, o):
        layer, r0, size = pieces[g]
        return pltpu.make_async_remote_copy(
            src_ref=pack.at[layer, o - 1, :, pl.ds(r0, size), :],
            dst_ref=land[g].at[pl.ds(SLOTS * mycol, SLOTS)],
            send_sem=csend.at[g, o],
            recv_sem=crecv.at[g, o],
            device_id={"col": target_of(o)},
            device_id_type=MESH,
        )

    def relay_copy(o):
        return pltpu.make_async_remote_copy(
            src_ref=zpack.at[o - 1],
            dst_ref=zland.at[pl.ds(SLOTS * mycol, SLOTS)],
            send_sem=rsend.at[o],
            recv_sem=rrecv.at[o],
            device_id={"col": target_of(o)},
            device_id_type=MESH,
        )

    def row_copy(g, zb, cb, way, target):
        layer, r0, size = pieces[g]
        block = zb * CORES + cb
        ref = layer_ref(layer).at[:, pl.ds(pl.multiple_of(block * rows + r0, TILE), size), :]
        return pltpu.make_async_remote_copy(
            src_ref=ref,
            dst_ref=ref,
            send_sem=zsend.at[g, zb, way],
            recv_sem=zrecv.at[g, block],
            device_id={"row": target},
            device_id_type=MESH,
        )

    def near_copy(cb):
        start = pl.multiple_of((near * CORES + cb) * rows, TILE)
        ref = full.at[0, :, pl.ds(start, rows), :]
        return pltpu.make_async_remote_copy(
            src_ref=ref,
            dst_ref=ref,
            send_sem=psend.at[0],
            recv_sem=precv.at[0],
            device_id={"row": partner},
            device_id_type=MESH,
        )

    def most_of(block):
        return jnp.max(block.reshape(-1, TILE, HDIM), axis=0)

    def fill(from_ref, out_ref, land_ref):
        for j in range(SLOTS):
            land_ref[SLOTS * mycol + j] = from_ref[table[j]]

        @pl.loop(1, cols)
        def _(o):
            for j in range(SLOTS):
                out_ref[o - 1, j] = from_ref[table[o * SLOTS + j]]

        @pl.loop(1, cols)
        def _(o):
            for j in range(SLOTS):
                guard[j] = most_of(out_ref[o - 1, j])

    def select(land_ref, layer, start, size):
        ref = layer_ref(layer)

        @pl.loop(0, heads)
        def _(t):
            ref[t, pl.ds(start, size), :] = land_ref[table[cols * SLOTS + t]]

        @pl.loop(0, heads)
        def _(t):
            guard[t] = most_of(ref[t, pl.ds(start, size), :])

    def hand_out(g):
        layer, r0, size = pieces[g]
        fill(own[g], pack.at[layer, :, :, pl.ds(r0, size), :], land[g])
        for o in range(1, cols):
            col_copy(g, o).start()

    def wait_own(g):
        for head in range(heads):
            own_copy(g, head).wait()

    def down_goes(g):
        return z > 1 if pieces[g][0] == 0 else has_down

    def up_goes(g):
        return z < zs - 2 if pieces[g][0] == 0 else has_up

    def stage_own(g):
        layer, r0, size = pieces[g]
        for o in range(1, cols):
            col_copy(g, o).wait_recv()
        select(land[g], layer, pl.multiple_of(me * rows + r0, TILE), size)

        @pl.when(down_goes(g))
        def _():
            row_copy(g, z, core, 0, down).start()

        @pl.when(up_goes(g))
        def _():
            row_copy(g, z, core, 1, up).start()

        row_copy(g, z, core, 2, partner).start()

    def stage_forward(g):
        for h in range(1, zs):
            raw = pieces[g][0] == 0 and h == 1

            @pl.when((z + h < zs) & (z > 0) if raw else z + h < zs)
            def _():
                row_copy(g, z + h, core, 0, down).wait_recv()

                @pl.when(has_down)
                def _():
                    row_copy(g, z + h, core, 0, down).start()

                row_copy(g, z + h, core, 2, partner).start()

            @pl.when((z - h >= 0) & (z < zs - 1) if raw else z - h >= 0)
            def _():
                row_copy(g, z - h, core, 1, up).wait_recv()

                @pl.when(has_up)
                def _():
                    row_copy(g, z - h, core, 1, up).start()

                row_copy(g, z - h, core, 2, partner).start()

    def relay_out():
        @pl.when(is_end)
        def _():
            for g in first:
                raw_copy(g, 0, down).wait_recv()
            fill(zown, zpack, zland)
            for o in range(1, cols):
                relay_copy(o).start()

    def relay_in():
        @pl.when(is_end)
        def _():
            for o in range(1, cols):
                relay_copy(o).wait_recv()
            select(zland, 0, pl.multiple_of((near * CORES + core) * rows, TILE), rows)
            near_copy(core).start()

    def wait_partner(layer):
        for g in range(count):
            if pieces[g][0] != layer:
                continue

            @pl.loop(0, zs)
            def _(zb):
                if layer == 0:
                    @pl.when(jnp.logical_not(is_end & (zb == near)))
                    def _():
                        row_copy(g, zb, 1 - core, 2, partner).wait_recv()
                else:
                    row_copy(g, zb, 1 - core, 2, partner).wait_recv()

        if layer == 0:
            @pl.when(is_end)
            def _():
                near_copy(1 - core).wait_recv()

    def compute(layer):
        for t0 in range(0, heads, 2):
            pair = (t0, t0 + 1)

            def read(t, at):
                return full[layer, t, at, :]

            def write(i, at, both):
                codes_refs[layer][at, pl.ds(t0 * HDIM, 2 * HDIM)] = both

            tops = tops_of(read, width, pair)
            note_tops(peaks_ref, layer, pair, tops)
            checked_ref[layer, :, pl.ds(t0 * HDIM, 2 * HDIM)] = project(
                read, write, pbuf, tops, width, pair
            ).astype(checked_ref.dtype)

    for g in first:
        wait_own(g)

        @pl.when(z == 1)
        def _():
            raw_copy(g, 0, down).start()

        @pl.when(z == zs - 2)
        def _():
            raw_copy(g, 1, up).start()

    sent = 0

    def hand_out_layer(layer):
        for g in range(count):
            if pieces[g][0] == layer:
                if layer > 0:
                    wait_own(g)
                hand_out(g)

    hand_out_layer(0)
    hand_out_layer(1)
    stage_own(0)
    stage_own(1)
    for g in range(count):
        stage_forward(g)
        if g + 2 < count:
            stage_own(g + 2)
        if g + 2 == first[-1]:
            relay_out()
            for layer in range(2, layers):
                hand_out_layer(layer)
        layer = pieces[g][0]
        if layer > 0 and pieces[g - 1][0] != layer:
            if layer == 1:
                relay_in()
                probe_copy.wait()
            wait_partner(layer - 1)
            compute(layer - 1)
    wait_partner(layers - 1)

    for g in first:
        @pl.when(z == 1)
        def _():
            raw_copy(g, 0, down).wait_send()

        @pl.when(z == zs - 2)
        def _():
            raw_copy(g, 1, up).wait_send()

    for g in range(count):
        for o in range(1, cols):
            col_copy(g, o).wait_send()

        @pl.loop(0, zs)
        def _(zb):
            goes_down, goes_up = down_goes(g), up_goes(g)

            @pl.when((has_down & (zb > z)) | (goes_down & (zb == z)))
            def _():
                row_copy(g, zb, core, 0, down).wait_send()

            @pl.when((has_up & (zb < z)) | (goes_up & (zb == z)))
            def _():
                row_copy(g, zb, core, 1, up).wait_send()

            if pieces[g][0] == 0:
                @pl.when(jnp.logical_not(is_end & (zb == near)))
                def _():
                    row_copy(g, zb, core, 2, partner).wait_send()
            else:
                row_copy(g, zb, core, 2, partner).wait_send()

    @pl.when(is_end)
    def _():
        for o in range(1, cols):
            relay_copy(o).wait_send()
        near_copy(core).wait_send()


def finish_kernel(
    checked_ref, last_ref, pbuf, peaks_ref, *refs,
):
    done = checked_ref.shape[0]
    codes_refs, refs = refs[:done], refs[done:]
    (
        codes_out, checked_out, peaks_out,
        cbuf, kbuf, tops_ref, codesem, stepsem, checksem, peaksem,
    ) = refs
    heads, width, _ = last_ref.shape
    steps = width // KSTEP
    half = width // 2
    copies = []
    for layer in range(done):
        for i in range(2):
            at = pl.ds(i * half, half)
            copies.append(
                pltpu.make_async_copy(
                    codes_refs[layer].at[at], codes_out.at[layer, at], codesem.at[layer, i]
                )
            )
    copies.append(
        pltpu.make_async_copy(checked_ref, checked_out.at[pl.ds(0, done)], checksem.at[0])
    )
    for copy in copies:
        copy.start()
    tops_ref[...] = peaks_ref[...]

    def step_copy(k, i):
        at = pl.ds(pl.multiple_of(i * KSTEP, KSTEP), KSTEP)
        lanes = pl.ds(k * 2 * HDIM, 2 * HDIM)
        return pltpu.make_async_copy(
            cbuf.at[at, lanes], codes_out.at[done, at, lanes], stepsem.at[k, i]
        )

    def read(t, at):
        return last_ref[t, at, :]

    for t0 in range(0, heads, 2):
        pair = (t0, t0 + 1)

        def write(i, at, both):
            cbuf[at, pl.ds(t0 * HDIM, 2 * HDIM)] = both
            step_copy(t0 // 2, i).start()

        tops = tops_of(read, width, pair)
        note_tops(tops_ref, done, pair, tops)
        kbuf[:, pl.ds(t0 * HDIM, 2 * HDIM)] = project(
            read, write, pbuf, tops, width, pair
        ).astype(kbuf.dtype)
    ends = [
        pltpu.make_async_copy(kbuf, checked_out.at[done], checksem.at[1]),
        pltpu.make_async_copy(tops_ref, peaks_out, peaksem.at[0]),
    ]
    for copy in ends:
        copy.start()
    for copy in copies + ends:
        copy.wait()
    for k in range(heads // 2):
        @pl.loop(0, steps)
        def _(i):
            step_copy(k, i).wait()


def per_device(train_weight, src_map, tgt_map, probe):
    cols = lax.axis_size("col")
    zs = lax.axis_size("row") // CORES
    layers, rows, span = train_weight.shape
    heads = src_map.shape[0] // cols
    tokens, width = probe.shape
    pieces = piece_list(layers, rows)
    count, done = len(pieces), layers - 1
    dtype = train_weight.dtype
    others = cols - 1
    anywhere = pl.BlockSpec(memory_space=pl.ANY)
    vmem = pl.BlockSpec(memory_space=pltpu.VMEM)
    dma = pltpu.SemaphoreType.DMA
    block = 2 * rows * HDIM
    grant = block * (
        done * heads * 2 * zs
        + layers * SLOTS * others
        + heads + SLOTS * others + SLOTS * cols
        + layers * (heads + SLOTS * cols)
    ) + 2**21
    gathered = pl.pallas_call(
        functools.partial(gather_kernel, pieces, zs, cols),
        out_shape=(
            pltpu.VMEM((done, tokens, span), dtype),
            pltpu.VMEM((heads, width, HDIM), dtype),
            pltpu.VMEM((tokens, width), dtype),
            pltpu.VMEM((layers, heads), jnp.float32),
        )
        + (pltpu.VMEM((width, span), dtype),) * done,
        in_specs=[pl.BlockSpec(memory_space=pltpu.SMEM)] * 2 + [anywhere] * 2,
        out_specs=(vmem,) * (4 + done),
        scratch_shapes=[
            pltpu.VMEM((done, heads, width, HDIM), dtype),
            pltpu.VMEM((layers, others, SLOTS, rows, HDIM), dtype),
            pltpu.VMEM((heads, rows, HDIM), dtype),
            pltpu.VMEM((others, SLOTS, rows, HDIM), dtype),
            pltpu.VMEM((cols * SLOTS, rows, HDIM), dtype),
            pltpu.VMEM((heads, TILE, HDIM), dtype),
            pltpu.SMEM((cols * SLOTS + heads,), jnp.int32),
            dma((count, heads)),
            dma((1,)),
            dma((count, cols)),
            dma((count, cols)),
            dma((count, zs, 3)),
            dma((count, zs * CORES)),
            dma((count, 2)),
            dma((count,)),
            dma((cols,)),
            dma((cols,)),
            dma((1,)),
            dma((1,)),
        ]
        + [pltpu.VMEM((heads, size, HDIM), dtype) for _, _, size in pieces]
        + [pltpu.VMEM((cols * SLOTS, size, HDIM), dtype) for _, _, size in pieces],
        compiler_params=pltpu.CompilerParams(
            collective_id=0, has_side_effects=True, vmem_limit_bytes=grant
        ),
    )(src_map, tgt_map, train_weight, probe)
    codes, checked, peaks = pl.pallas_call(
        finish_kernel,
        out_shape=(
            jax.ShapeDtypeStruct((layers, width, span), dtype),
            jax.ShapeDtypeStruct((layers, tokens, span), dtype),
            jax.ShapeDtypeStruct((layers, heads), jnp.float32),
        ),
        in_specs=[vmem] * (4 + done),
        out_specs=(anywhere,) * 3,
        scratch_shapes=[
            pltpu.VMEM((width, span), dtype),
            pltpu.VMEM((tokens, span), dtype),
            pltpu.VMEM((layers, heads), jnp.float32),
            dma((done, 2)),
            dma((heads // 2, width // KSTEP)),
            dma((2,)),
            dma((1,)),
        ],
        compiler_params=pltpu.CompilerParams(
            vmem_limit_bytes=2 * width * span + 2 * tokens * span + 2**22
        ),
    )(*[pltpu.with_memory_space_constraint(x, pltpu.VMEM) for x in gathered])
    return codes, peaks, checked


def solution(mesh):
    in_specs = (P(None, "row", "col"), P(), P(), P("row", None))
    out_specs = (P(None, None, "col"), P(None, "col"), P(None, "row", "col"))
    return jax.shard_map(
        per_device, mesh=mesh, in_specs=in_specs, out_specs=out_specs, check_vma=False
    )
```

```python
import functools

import jax
import jax.numpy as jnp
from jax import lax
from jax.experimental import pallas as pl
from jax.experimental.pallas import tpu as pltpu
from jax.sharding import PartitionSpec as P

HDIM = 128
CORES = 2
TILE = 16
PSTEP = 128
CSTEP = 512
KSTEP = 4608
NSTEP = 256
SLOTS = 2
MESH = pl.DeviceIdType.MESH


def split(rows, shares):
    units, total = rows // TILE, sum(shares)
    cuts = [units * sum(shares[:i]) // total for i in range(len(shares) + 1)]
    return [(a * TILE, (b - a) * TILE) for a, b in zip(cuts, cuts[1:]) if b > a]


def piece_list(layers, rows):
    out = []
    for layer in range(layers):
        shares = (1, 2, 3, 6) if layer == 0 else ((3, 2, 1) if layer == layers - 1 else (1, 1))
        out.extend((layer, r0, size) for r0, size in split(rows, shares))
    return out


def peaks_of(read, width, heads):
    def most(i, acc):
        at = pl.ds(pl.multiple_of(i * PSTEP, PSTEP), PSTEP)
        return tuple(
            jnp.maximum(a, jnp.max(jnp.abs(read(t, at)).reshape(-1, TILE, HDIM), axis=0))
            for t, a in enumerate(acc)
        )

    zero = jnp.zeros((TILE, HDIM), jnp.bfloat16)
    best = lax.fori_loop(0, width // PSTEP, most, (zero,) * heads)
    return [
        jnp.max(jnp.max(b.astype(jnp.float32), axis=0, keepdims=True), axis=1, keepdims=True)
        for b in best
    ]


def encode(read, write, tops, width):
    spread = [jnp.broadcast_to(p, (1, HDIM)) for p in tops]
    inverse = [1.0 / ((p + 1e-06) * 0.25) for p in spread]

    @pl.loop(0, width // CSTEP)
    def _(i):
        at = pl.ds(pl.multiple_of(i * CSTEP, CSTEP), CSTEP)
        for t, inv in enumerate(inverse):
            scaled = (read(t, at) * 0.25).astype(jnp.float32) * inv
            write(i, t, at, scaled.astype(jnp.bfloat16))


def project(codes_ref, pbuf, out_ref, tops):
    width, span = codes_ref.shape
    tokens = pbuf.shape[0]
    spread = jnp.concatenate([jnp.broadcast_to(p, (1, HDIM)) for p in tops], axis=1)
    for n0 in range(0, span, NSTEP):
        lanes = pl.ds(n0, NSTEP)

        def step(i, acc):
            at = pl.ds(pl.multiple_of(i * KSTEP, KSTEP), KSTEP)
            return acc + jnp.dot(
                pbuf[:, at], codes_ref[at, lanes], preferred_element_type=jnp.float32
            )

        acc = lax.fori_loop(0, width // KSTEP, step, jnp.zeros((tokens, NSTEP), jnp.float32))
        out_ref[:, lanes] = (acc * spread[:, n0 : n0 + NSTEP]).astype(out_ref.dtype)


def note_tops(peaks_ref, layer, tops):
    here = lax.broadcasted_iota(jnp.int32, peaks_ref.shape, 0) == layer
    lane = lax.broadcasted_iota(jnp.int32, peaks_ref.shape, 1)
    for t, top in enumerate(tops):
        peaks_ref[...] = jnp.where(here & (lane == t), top, peaks_ref[...])


def gather_kernel(
    pieces, zs, cols, src_hbm, tgt_hbm, w_ref, probe_ref,
    checked_ref, last_ref, pbuf, peaks_ref, *refs,
):
    layers, rows, _ = w_ref.shape
    codes_refs, refs = refs[: layers - 1], refs[layers - 1 :]
    (
        full, pack, zown, zpack, zland, guard, table, src_map, tgt_map,
        mapsem, local, probesem, csend, crecv, zsend, zrecv,
        rawsend, rawrecv, rsend, rrecv, psend, precv, *bufs,
    ) = refs
    count = len(pieces)
    own, land = bufs[:count], bufs[count:]
    heads, width, _ = last_ref.shape
    me = lax.axis_index("row")
    mycol = lax.axis_index("col")
    z = me // CORES
    core = me % CORES
    partner = z * CORES + (1 - core)
    down, up = me - CORES, me + CORES
    has_down, has_up = z > 0, z < zs - 1
    low, high = z == 0, z == zs - 1
    is_end = low | high
    near = jnp.where(low, 1, zs - 2)
    first = [g for g in range(count) if pieces[g][0] == 0]

    def layer_ref(layer):
        return last_ref if layer == layers - 1 else full.at[layer]

    def own_copy(g, head):
        layer, r0, size = pieces[g]
        return pltpu.make_async_copy(
            w_ref.at[layer, pl.ds(r0, size), pl.ds(head * HDIM, HDIM)],
            own[g].at[head],
            local.at[g, head],
        )

    def target_of(o):
        return lax.rem(mycol + cols - o, cols)

    map_copies = [
        pltpu.make_async_copy(src_hbm, src_map, mapsem.at[0]),
        pltpu.make_async_copy(tgt_hbm, tgt_map, mapsem.at[1]),
    ]
    for copy in map_copies:
        copy.start()
    barrier = pltpu.get_barrier_semaphore()
    for o in range(1, cols):
        pl.semaphore_signal(barrier, inc=1, device_id={"col": target_of(o)}, device_id_type=MESH)
    pl.semaphore_signal(barrier, inc=1, device_id={"row": partner}, device_id_type=MESH)

    @pl.when(has_down)
    def _():
        pl.semaphore_signal(barrier, inc=1, device_id={"row": down}, device_id_type=MESH)

    @pl.when(has_up)
    def _():
        pl.semaphore_signal(barrier, inc=1, device_id={"row": up}, device_id_type=MESH)

    for g in range(count):
        for head in range(heads):
            own_copy(g, head).start()
    probe_copy = pltpu.make_async_copy(probe_ref, pbuf, probesem.at[0])
    probe_copy.start()
    peaks_ref[...] = jnp.zeros_like(peaks_ref)

    for copy in map_copies:
        copy.wait()
    total = cols * heads
    mine = [src_map[mycol * heads + s] for s in range(heads)]
    want = [tgt_map[mycol * heads + t] for t in range(heads)]
    goes = [jnp.int32(0)] * heads
    for p in range(heads, total):
        wanted = tgt_map[p]
        goes = [g + jnp.where(m == wanted, p // heads, 0) for g, m in zip(goes, mine)]
    for o in range(cols):
        to = target_of(o)
        seen, picks = jnp.int32(0), [jnp.int32(0)] * SLOTS
        for s in range(heads):
            hit = goes[s] == to
            picks = [jnp.where(hit & (seen == j), s, q) for j, q in enumerate(picks)]
            seen = seen + jnp.where(hit, 1, 0)
        for j in range(SLOTS):
            table[o * SLOTS + j] = picks[j]
    slot_of = [jnp.int32(0)] * heads
    for c in range(cols):
        seen = jnp.int32(0)
        for s in range(heads):
            held = src_map[c * heads + s]
            for t in range(heads):
                slot_of[t] = jnp.where(want[t] == held, c * SLOTS + seen, slot_of[t])
            hit = want[0] == held
            for t in range(1, heads):
                hit = hit | (want[t] == held)
            seen = jnp.minimum(seen + jnp.where(hit, 1, 0), SLOTS - 1)
    for t in range(heads):
        table[cols * SLOTS + t] = slot_of[t]

    pl.semaphore_wait(barrier, cols + has_down.astype(jnp.int32) + has_up.astype(jnp.int32))

    def raw_copy(g, way, target):
        _, r0, size = pieces[g]
        return pltpu.make_async_remote_copy(
            src_ref=own[g],
            dst_ref=zown.at[:, pl.ds(r0, size), :],
            send_sem=rawsend.at[g, way],
            recv_sem=rawrecv.at[g],
            device_id={"row": target},
            device_id_type=MESH,
        )

    def col_copy(g, o):
        layer, r0, size = pieces[g]
        return pltpu.make_async_remote_copy(
            src_ref=pack.at[layer, o - 1, :, pl.ds(r0, size), :],
            dst_ref=land[g].at[pl.ds(SLOTS * mycol, SLOTS)],
            send_sem=csend.at[g, o],
            recv_sem=crecv.at[g, o],
            device_id={"col": target_of(o)},
            device_id_type=MESH,
        )

    def relay_copy(o):
        return pltpu.make_async_remote_copy(
            src_ref=zpack.at[o - 1],
            dst_ref=zland.at[pl.ds(SLOTS * mycol, SLOTS)],
            send_sem=rsend.at[o],
            recv_sem=rrecv.at[o],
            device_id={"col": target_of(o)},
            device_id_type=MESH,
        )

    def row_copy(g, zb, cb, way, target):
        layer, r0, size = pieces[g]
        block = zb * CORES + cb
        ref = layer_ref(layer).at[:, pl.ds(pl.multiple_of(block * rows + r0, TILE), size), :]
        return pltpu.make_async_remote_copy(
            src_ref=ref,
            dst_ref=ref,
            send_sem=zsend.at[g, zb, way],
            recv_sem=zrecv.at[g, block],
            device_id={"row": target},
            device_id_type=MESH,
        )

    def near_copy(cb):
        start = pl.multiple_of((near * CORES + cb) * rows, TILE)
        ref = full.at[0, :, pl.ds(start, rows), :]
        return pltpu.make_async_remote_copy(
            src_ref=ref,
            dst_ref=ref,
            send_sem=psend.at[0],
            recv_sem=precv.at[0],
            device_id={"row": partner},
            device_id_type=MESH,
        )

    def most_of(block):
        return jnp.max(block.reshape(-1, TILE, HDIM), axis=0)

    def fill(from_ref, out_ref, land_ref):
        for j in range(SLOTS):
            land_ref[SLOTS * mycol + j] = from_ref[table[j]]

        @pl.loop(1, cols)
        def _(o):
            for j in range(SLOTS):
                out_ref[o - 1, j] = from_ref[table[o * SLOTS + j]]

        @pl.loop(1, cols)
        def _(o):
            for j in range(SLOTS):
                guard[j] = most_of(out_ref[o - 1, j])

    def select(land_ref, layer, start, size):
        ref = layer_ref(layer)

        @pl.loop(0, heads)
        def _(t):
            ref[t, pl.ds(start, size), :] = land_ref[table[cols * SLOTS + t]]

        @pl.loop(0, heads)
        def _(t):
            guard[t] = most_of(ref[t, pl.ds(start, size), :])

    def hand_out(g):
        layer, r0, size = pieces[g]
        fill(own[g], pack.at[layer, :, :, pl.ds(r0, size), :], land[g])
        for o in range(1, cols):
            col_copy(g, o).start()

    def wait_own(g):
        for head in range(heads):
            own_copy(g, head).wait()

    def down_goes(g):
        return z > 1 if pieces[g][0] == 0 else has_down

    def up_goes(g):
        return z < zs - 2 if pieces[g][0] == 0 else has_up

    def stage_own(g):
        layer, r0, size = pieces[g]
        for o in range(1, cols):
            col_copy(g, o).wait_recv()
        select(land[g], layer, pl.multiple_of(me * rows + r0, TILE), size)

        @pl.when(down_goes(g))
        def _():
            row_copy(g, z, core, 0, down).start()

        @pl.when(up_goes(g))
        def _():
            row_copy(g, z, core, 1, up).start()

        row_copy(g, z, core, 2, partner).start()

    def stage_forward(g):
        for h in range(1, zs):
            raw = pieces[g][0] == 0 and h == 1

            @pl.when((z + h < zs) & (z > 0) if raw else z + h < zs)
            def _():
                row_copy(g, z + h, core, 0, down).wait_recv()

                @pl.when(has_down)
                def _():
                    row_copy(g, z + h, core, 0, down).start()

                row_copy(g, z + h, core, 2, partner).start()

            @pl.when((z - h >= 0) & (z < zs - 1) if raw else z - h >= 0)
            def _():
                row_copy(g, z - h, core, 1, up).wait_recv()

                @pl.when(has_up)
                def _():
                    row_copy(g, z - h, core, 1, up).start()

                row_copy(g, z - h, core, 2, partner).start()

    def relay_out(_):
        for g in first:
            raw_copy(g, 0, down).wait_recv()
        fill(zown, zpack, zland)
        for o in range(1, cols):
            relay_copy(o).start()

    def relay_in(_):
        for o in range(1, cols):
            relay_copy(o).wait_recv()
        select(zland, 0, pl.multiple_of((near * CORES + core) * rows, TILE), rows)
        near_copy(core).start()

    def wait_partner(layer):
        for g in range(count):
            if pieces[g][0] != layer:
                continue

            @pl.loop(0, zs)
            def _(zb):
                if layer == 0:
                    @pl.when(jnp.logical_not(is_end & (zb == near)))
                    def _():
                        row_copy(g, zb, 1 - core, 2, partner).wait_recv()
                else:
                    row_copy(g, zb, 1 - core, 2, partner).wait_recv()

        if layer == 0:
            @pl.when(is_end)
            def _():
                near_copy(1 - core).wait_recv()

    def compute(layer):
        codes_ref = codes_refs[layer]

        def read(t, at):
            return full[layer, t, at, :]

        def write(i, t, at, codes):
            codes_ref[at, pl.ds(t * HDIM, HDIM)] = codes

        tops = peaks_of(read, width, heads)
        note_tops(peaks_ref, layer, tops)
        encode(read, write, tops, width)
        project(codes_ref, pbuf, checked_ref.at[layer], tops)

    for g in first:
        wait_own(g)

        @pl.when(z == 1)
        def _():
            raw_copy(g, 0, down).start()

        @pl.when(z == zs - 2)
        def _():
            raw_copy(g, 1, up).start()

    def hand_out_layer(layer):
        for g in range(count):
            if pieces[g][0] == layer:
                if layer > 0:
                    wait_own(g)
                hand_out(g)

    def run(steps):
        for stage, g in steps:
            stage(g)

    def either(ends, mids):
        @pl.when(is_end)
        def _():
            run(ends)

        @pl.when(jnp.logical_not(is_end))
        def _():
            run(mids)

    def finish(layer):
        if layer == 0:
            probe_copy.wait()
        wait_partner(layer)
        compute(layer)

    def of(layer, stage):
        return [(stage, g) for g in range(count) if pieces[g][0] == layer]

    hand_out_layer(0)
    hand_out_layer(1)
    own0, fwd0 = of(0, stage_own), of(0, stage_forward)
    own1, fwd1 = of(1, stage_own), of(1, stage_forward)
    lead = own0[:2]
    for f, o in zip(fwd0, own0[2:] + own1):
        lead += [f, o]
    cut = 2 * len(own0) - 2
    either(own0 + [(relay_out, 0)], lead[:cut])
    for layer in range(2, layers):
        hand_out_layer(layer)
    started = lead[cut:] + fwd0[len(own0) - 2 + len(own1):]
    rest = [o for o in own1 if o not in lead]
    either(own1 + fwd0 + [(relay_in, 0)], started + rest)
    finish(0)
    later = []
    for layer in range(2, layers):
        later += of(layer, stage_own)
    ahead = len(of(2, stage_own))
    either(later + fwd1, fwd1[:1] + later[:ahead] + fwd1[1:] + later[ahead:])
    finish(1)
    for layer in range(2, layers):
        run(of(layer, stage_forward))
        if layer < layers - 1:
            finish(layer)
    wait_partner(layers - 1)

    for g in first:
        @pl.when(z == 1)
        def _():
            raw_copy(g, 0, down).wait_send()

        @pl.when(z == zs - 2)
        def _():
            raw_copy(g, 1, up).wait_send()

    for g in range(count):
        for o in range(1, cols):
            col_copy(g, o).wait_send()

        @pl.loop(0, zs)
        def _(zb):
            goes_down, goes_up = down_goes(g), up_goes(g)

            @pl.when((has_down & (zb > z)) | (goes_down & (zb == z)))
            def _():
                row_copy(g, zb, core, 0, down).wait_send()

            @pl.when((has_up & (zb < z)) | (goes_up & (zb == z)))
            def _():
                row_copy(g, zb, core, 1, up).wait_send()

            if pieces[g][0] == 0:
                @pl.when(jnp.logical_not(is_end & (zb == near)))
                def _():
                    row_copy(g, zb, core, 2, partner).wait_send()
            else:
                row_copy(g, zb, core, 2, partner).wait_send()

    @pl.when(is_end)
    def _():
        for o in range(1, cols):
            relay_copy(o).wait_send()
        near_copy(core).wait_send()


def finish_kernel(
    checked_ref, last_ref, pbuf, peaks_ref, *refs,
):
    done = checked_ref.shape[0]
    codes_refs, refs = refs[:done], refs[done:]
    (
        codes_out, checked_out, peaks_out,
        cbuf, kbuf, tops_ref, codesem, stepsem, checksem, peaksem,
    ) = refs
    heads, width, _ = last_ref.shape
    half = width // 2
    copies = []
    for layer in range(done):
        for i in range(2):
            at = pl.ds(i * half, half)
            copies.append(
                pltpu.make_async_copy(
                    codes_refs[layer].at[at], codes_out.at[layer, at], codesem.at[layer, i]
                )
            )
    copies.append(
        pltpu.make_async_copy(checked_ref, checked_out.at[pl.ds(0, done)], checksem.at[0])
    )
    for copy in copies:
        copy.start()
    tops_ref[...] = peaks_ref[...]

    def step_copy(i):
        at = pl.ds(pl.multiple_of(i * CSTEP, CSTEP), CSTEP)
        return pltpu.make_async_copy(cbuf.at[at], codes_out.at[done, at], stepsem.at[i])

    def read(t, at):
        return last_ref[t, at, :]

    def write(i, t, at, codes):
        cbuf[at, pl.ds(t * HDIM, HDIM)] = codes
        if t == heads - 1:
            step_copy(i).start()

    tops = peaks_of(read, width, heads)
    note_tops(tops_ref, done, tops)
    encode(read, write, tops, width)
    project(cbuf, pbuf, kbuf, tops)
    ends = [
        pltpu.make_async_copy(kbuf, checked_out.at[done], checksem.at[1]),
        pltpu.make_async_copy(tops_ref, peaks_out, peaksem.at[0]),
    ]
    for copy in ends:
        copy.start()
    for copy in copies + ends:
        copy.wait()

    @pl.loop(0, width // CSTEP)
    def _(i):
        step_copy(i).wait()


def finish(gathered, layers, heads, width, span, tokens, dtype):
    done = layers - 1
    anywhere = pl.BlockSpec(memory_space=pl.ANY)
    vmem = pl.BlockSpec(memory_space=pltpu.VMEM)
    dma = pltpu.SemaphoreType.DMA
    codes, checked, peaks = pl.pallas_call(
        finish_kernel,
        out_shape=(
            jax.ShapeDtypeStruct((layers, width, span), dtype),
            jax.ShapeDtypeStruct((layers, tokens, span), dtype),
            jax.ShapeDtypeStruct((layers, heads), jnp.float32),
        ),
        in_specs=[vmem] * (4 + done),
        out_specs=(anywhere,) * 3,
        scratch_shapes=[
            pltpu.VMEM((width, span), dtype),
            pltpu.VMEM((tokens, span), dtype),
            pltpu.VMEM((layers, heads), jnp.float32),
            dma((done, 2)),
            dma((width // CSTEP,)),
            dma((2,)),
            dma((1,)),
        ],
        compiler_params=pltpu.CompilerParams(
            vmem_limit_bytes=2 * width * span + 2 * tokens * span + 2**22
        ),
    )(*[pltpu.with_memory_space_constraint(x, pltpu.VMEM) for x in gathered])
    return codes, peaks, checked


def per_device(train_weight, src_map, tgt_map, probe):
    cols = lax.axis_size("col")
    zs = lax.axis_size("row") // CORES
    layers, rows, span = train_weight.shape
    heads = src_map.shape[0] // cols
    tokens, width = probe.shape
    pieces = piece_list(layers, rows)
    count, done = len(pieces), layers - 1
    dtype = train_weight.dtype
    others = cols - 1
    anywhere = pl.BlockSpec(memory_space=pl.ANY)
    vmem = pl.BlockSpec(memory_space=pltpu.VMEM)
    dma = pltpu.SemaphoreType.DMA
    block = 2 * rows * HDIM
    grant = block * (
        done * heads * 2 * zs
        + layers * SLOTS * others
        + heads + SLOTS * others + SLOTS * cols
        + layers * (heads + SLOTS * cols)
    ) + 2**21
    maps = [pltpu.with_memory_space_constraint(x, pltpu.HBM) for x in (src_map, tgt_map)]
    gathered = pl.pallas_call(
        functools.partial(gather_kernel, pieces, zs, cols),
        out_shape=(
            pltpu.VMEM((done, tokens, span), dtype),
            pltpu.VMEM((heads, width, HDIM), dtype),
            pltpu.VMEM((tokens, width), dtype),
            pltpu.VMEM((layers, heads), jnp.float32),
        )
        + (pltpu.VMEM((width, span), dtype),) * done,
        in_specs=[pl.BlockSpec(memory_space=pltpu.HBM)] * 2 + [anywhere] * 2,
        out_specs=(vmem,) * (4 + done),
        scratch_shapes=[
            pltpu.VMEM((done, heads, width, HDIM), dtype),
            pltpu.VMEM((layers, others, SLOTS, rows, HDIM), dtype),
            pltpu.VMEM((heads, rows, HDIM), dtype),
            pltpu.VMEM((others, SLOTS, rows, HDIM), dtype),
            pltpu.VMEM((cols * SLOTS, rows, HDIM), dtype),
            pltpu.VMEM((heads, TILE, HDIM), dtype),
            pltpu.SMEM((cols * SLOTS + heads,), jnp.int32),
            pltpu.SMEM(src_map.shape, jnp.int32),
            pltpu.SMEM(tgt_map.shape, jnp.int32),
            dma((2,)),
            dma((count, heads)),
            dma((1,)),
            dma((count, cols)),
            dma((count, cols)),
            dma((count, zs, 3)),
            dma((count, zs * CORES)),
            dma((count, 2)),
            dma((count,)),
            dma((cols,)),
            dma((cols,)),
            dma((1,)),
            dma((1,)),
        ]
        + [pltpu.VMEM((heads, size, HDIM), dtype) for _, _, size in pieces]
        + [pltpu.VMEM((cols * SLOTS, size, HDIM), dtype) for _, _, size in pieces],
        compiler_params=pltpu.CompilerParams(
            collective_id=0, has_side_effects=True, vmem_limit_bytes=grant
        ),
    )(*maps, train_weight, probe)
    return finish(gathered, layers, heads, width, span, tokens, dtype)


def solution(mesh):
    in_specs = (P(None, "row", "col"), P(), P(), P("row", None))
    out_specs = (P(None, None, "col"), P(None, "col"), P(None, "row", "col"))
    return jax.shard_map(
        per_device, mesh=mesh, in_specs=in_specs, out_specs=out_specs, check_vma=False
    )
```

```python
import functools

import jax
import jax.numpy as jnp
from jax import lax
from jax.experimental import pallas as pl
from jax.experimental.pallas import tpu as pltpu
from jax.sharding import PartitionSpec as P

HDIM = 128
CORES = 2
TILE = 16
PSTEP = 128
CSTEP = 512
KSTEP = 4608
NSTEP = 256
SLOTS = 2
VMEM = 63 * 2**20
MESH = pl.DeviceIdType.MESH


def split(rows, shares):
    units, total = rows // TILE, sum(shares)
    cuts = [units * sum(shares[:i]) // total for i in range(len(shares) + 1)]
    return [(a * TILE, (b - a) * TILE) for a, b in zip(cuts, cuts[1:]) if b > a]


def piece_list(layers, rows):
    out = []
    for layer in range(layers):
        if layer == 0:
            shares = (1, 2, 3, 6)
        elif layer == layers - 1:
            shares = (3, 2, 1)
        else:
            shares = (1, 1) if layer == 1 else (1,)
        out.extend((layer, r0, size) for r0, size in split(rows, shares))
    return out


def raw_parts(pieces, raw):
    parts = {}
    for g in raw:
        layer, _, size = pieces[g]
        parts[layer] = parts.get(layer, 0) + size
    out, place = [], 0
    for layer, size in parts.items():
        out.append((layer, size, place))
        place += size
    return out


def peaks_of(read, width, heads):
    def most(i, acc):
        at = pl.ds(pl.multiple_of(i * PSTEP, PSTEP), PSTEP)
        return tuple(
            jnp.maximum(a, jnp.max(jnp.abs(read(t, at)).reshape(-1, TILE, HDIM), axis=0))
            for t, a in enumerate(acc)
        )

    zero = jnp.zeros((TILE, HDIM), jnp.bfloat16)
    best = lax.fori_loop(0, width // PSTEP, most, (zero,) * heads)
    return [
        jnp.max(jnp.max(b.astype(jnp.float32), axis=0, keepdims=True), axis=1, keepdims=True)
        for b in best
    ]


def encode(read, write, tops, width):
    spread = [jnp.broadcast_to(p, (1, HDIM)) for p in tops]
    inverse = [1.0 / ((p + 1e-06) * 0.25) for p in spread]

    @pl.loop(0, width // CSTEP)
    def _(i):
        at = pl.ds(pl.multiple_of(i * CSTEP, CSTEP), CSTEP)
        for t, inv in enumerate(inverse):
            scaled = (read(t, at) * 0.25).astype(jnp.float32) * inv
            write(i, t, at, scaled.astype(jnp.bfloat16))


def project(codes_ref, pbuf, out_ref, tops):
    width, span = codes_ref.shape
    tokens = pbuf.shape[0]
    spread = jnp.concatenate([jnp.broadcast_to(p, (1, HDIM)) for p in tops], axis=1)
    for n0 in range(0, span, NSTEP):
        lanes = pl.ds(n0, NSTEP)

        def step(i, acc):
            at = pl.ds(pl.multiple_of(i * KSTEP, KSTEP), KSTEP)
            return acc + jnp.dot(
                pbuf[:, at], codes_ref[at, lanes], preferred_element_type=jnp.float32
            )

        acc = lax.fori_loop(0, width // KSTEP, step, jnp.zeros((tokens, NSTEP), jnp.float32))
        out_ref[:, lanes] = (acc * spread[:, n0 : n0 + NSTEP]).astype(out_ref.dtype)


def note_tops(peaks_ref, layer, tops):
    here = lax.broadcasted_iota(jnp.int32, peaks_ref.shape, 0) == layer
    lane = lax.broadcasted_iota(jnp.int32, peaks_ref.shape, 1)
    for t, top in enumerate(tops):
        peaks_ref[...] = jnp.where(here & (lane == t), top, peaks_ref[...])


def gather_kernel(
    pieces, raw, zs, cols, src_hbm, tgt_hbm, w_ref, probe_ref,
    checked_ref, last_ref, pbuf, peaks_ref, *refs,
):
    layers, rows, _ = w_ref.shape
    codes_refs, refs = refs[: layers - 1], refs[layers - 1 :]
    (
        full, pack, zown, zpack, zland, guard, table, src_map, tgt_map,
        mapsem, local, probesem, csend, crecv, zsend, zrecv,
        rawsend, rawrecv, rsend, rrecv, psend, precv, *bufs,
    ) = refs
    count = len(pieces)
    own, land = bufs[:count], bufs[count:]
    heads, width, _ = last_ref.shape
    me = lax.axis_index("row")
    mycol = lax.axis_index("col")
    z = me // CORES
    core = me % CORES
    partner = z * CORES + (1 - core)
    down, up = me - CORES, me + CORES
    has_down, has_up = z > 0, z < zs - 1
    low, high = z == 0, z == zs - 1
    is_end = low | high
    near = jnp.where(low, 1, zs - 2)
    parts = raw_parts(pieces, raw)

    def layer_ref(layer):
        return last_ref if layer == layers - 1 else full.at[layer]

    def own_copy(g, head):
        layer, r0, size = pieces[g]
        return pltpu.make_async_copy(
            w_ref.at[layer, pl.ds(r0, size), pl.ds(head * HDIM, HDIM)],
            own[g].at[head],
            local.at[g, head],
        )

    def target_of(o):
        return lax.rem(mycol + cols - o, cols)

    barrier = pltpu.get_barrier_semaphore()
    for o in range(1, cols):
        pl.semaphore_signal(barrier, inc=1, device_id={"col": target_of(o)}, device_id_type=MESH)
    pl.semaphore_signal(barrier, inc=1, device_id={"row": partner}, device_id_type=MESH)

    @pl.when(has_down)
    def _():
        pl.semaphore_signal(barrier, inc=1, device_id={"row": down}, device_id_type=MESH)

    @pl.when(has_up)
    def _():
        pl.semaphore_signal(barrier, inc=1, device_id={"row": up}, device_id_type=MESH)

    for g in raw:
        for head in range(heads):
            own_copy(g, head).start()
    map_copies = [
        pltpu.make_async_copy(src_hbm, src_map, mapsem.at[0]),
        pltpu.make_async_copy(tgt_hbm, tgt_map, mapsem.at[1]),
    ]
    for copy in map_copies:
        copy.start()
    for g in range(len(raw), count):
        for head in range(heads):
            own_copy(g, head).start()
    probe_copy = pltpu.make_async_copy(probe_ref, pbuf, probesem.at[0])
    probe_copy.start()
    peaks_ref[...] = jnp.zeros_like(peaks_ref)

    pl.semaphore_wait(barrier, cols + has_down.astype(jnp.int32) + has_up.astype(jnp.int32))

    def raw_copy(g, way, target):
        layer, r0, size = pieces[g]
        place = r0 + sum(n for other, n, _ in parts if other < layer)
        return pltpu.make_async_remote_copy(
            src_ref=own[g],
            dst_ref=zown.at[:, pl.ds(place, size), :],
            send_sem=rawsend.at[g, way],
            recv_sem=rawrecv.at[g],
            device_id={"row": target},
            device_id_type=MESH,
        )

    def col_copy(g, o):
        layer, r0, size = pieces[g]
        return pltpu.make_async_remote_copy(
            src_ref=pack.at[layer, o - 1, :, pl.ds(r0, size), :],
            dst_ref=land[g].at[pl.ds(SLOTS * mycol, SLOTS)],
            send_sem=csend.at[g, o],
            recv_sem=crecv.at[g, o],
            device_id={"col": target_of(o)},
            device_id_type=MESH,
        )

    def relay_copy(o):
        return pltpu.make_async_remote_copy(
            src_ref=zpack.at[o - 1],
            dst_ref=zland.at[pl.ds(SLOTS * mycol, SLOTS)],
            send_sem=rsend.at[o],
            recv_sem=rrecv.at[o],
            device_id={"col": target_of(o)},
            device_id_type=MESH,
        )

    def row_copy(g, zb, cb, way, target):
        layer, r0, size = pieces[g]
        block = zb * CORES + cb
        ref = layer_ref(layer).at[:, pl.ds(pl.multiple_of(block * rows + r0, TILE), size), :]
        return pltpu.make_async_remote_copy(
            src_ref=ref,
            dst_ref=ref,
            send_sem=zsend.at[g, zb, way],
            recv_sem=zrecv.at[g, block],
            device_id={"row": target},
            device_id_type=MESH,
        )

    def near_copy(k, cb):
        layer, size, _ = parts[k]
        start = pl.multiple_of((near * CORES + cb) * rows, TILE)
        ref = layer_ref(layer).at[:, pl.ds(start, size), :]
        return pltpu.make_async_remote_copy(
            src_ref=ref,
            dst_ref=ref,
            send_sem=psend.at[k],
            recv_sem=precv.at[k],
            device_id={"row": partner},
            device_id_type=MESH,
        )

    def most_of(block):
        return jnp.max(block.reshape(-1, TILE, HDIM), axis=0)

    def fill(from_ref, out_ref, land_ref):
        for j in range(SLOTS):
            land_ref[SLOTS * mycol + j] = from_ref[table[j]]

        @pl.loop(1, cols)
        def _(o):
            for j in range(SLOTS):
                out_ref[o - 1, j] = from_ref[table[o * SLOTS + j]]

        @pl.loop(1, cols)
        def _(o):
            for j in range(SLOTS):
                guard[j] = most_of(out_ref[o - 1, j])

    def select(land_ref, place, layer, start, size):
        ref = layer_ref(layer)

        @pl.loop(0, heads)
        def _(t):
            ref[t, pl.ds(start, size), :] = land_ref[table[cols * SLOTS + t], pl.ds(place, size), :]

        @pl.loop(0, heads)
        def _(t):
            guard[t] = most_of(ref[t, pl.ds(start, size), :])

    def hand_out(g):
        layer, r0, size = pieces[g]
        fill(own[g], pack.at[layer, :, :, pl.ds(r0, size), :], land[g])
        for o in range(1, cols):
            col_copy(g, o).start()

    def wait_own(g):
        for head in range(heads):
            own_copy(g, head).wait()

    def down_goes(g):
        return z > 1 if g in raw else has_down

    def up_goes(g):
        return z < zs - 2 if g in raw else has_up

    def stage_own(g):
        layer, r0, size = pieces[g]
        for o in range(1, cols):
            col_copy(g, o).wait_recv()
        select(land[g], 0, layer, pl.multiple_of(me * rows + r0, TILE), size)

        @pl.when(down_goes(g))
        def _():
            row_copy(g, z, core, 0, down).start()

        @pl.when(up_goes(g))
        def _():
            row_copy(g, z, core, 1, up).start()

        row_copy(g, z, core, 2, partner).start()

    def stage_forward(g):
        for h in range(1, zs):
            skips = g in raw and h == 1

            @pl.when((z + h < zs) & (z > 0) if skips else z + h < zs)
            def _():
                row_copy(g, z + h, core, 0, down).wait_recv()

                @pl.when(has_down)
                def _():
                    row_copy(g, z + h, core, 0, down).start()

                row_copy(g, z + h, core, 2, partner).start()

            @pl.when((z - h >= 0) & (z < zs - 1) if skips else z - h >= 0)
            def _():
                row_copy(g, z - h, core, 1, up).wait_recv()

                @pl.when(has_up)
                def _():
                    row_copy(g, z - h, core, 1, up).start()

                row_copy(g, z - h, core, 2, partner).start()

    def relay_out(_):
        for g in raw:
            raw_copy(g, 0, down).wait_recv()
        fill(zown, zpack, zland)
        for o in range(1, cols):
            relay_copy(o).start()

    def relay_in(_):
        for o in range(1, cols):
            relay_copy(o).wait_recv()
        start = pl.multiple_of((near * CORES + core) * rows, TILE)
        for k, (layer, size, place) in enumerate(parts):
            select(zland, place, layer, start, size)
            near_copy(k, core).start()

    def wait_partner(g):
        @pl.loop(0, zs)
        def _(zb):
            if g in raw:
                @pl.when(jnp.logical_not(is_end & (zb == near)))
                def _():
                    row_copy(g, zb, 1 - core, 2, partner).wait_recv()
            else:
                row_copy(g, zb, 1 - core, 2, partner).wait_recv()

    def drain(g):
        for o in range(1, cols):
            col_copy(g, o).wait_send()

        @pl.loop(0, zs)
        def _(zb):
            @pl.when((has_down & (zb > z)) | (down_goes(g) & (zb == z)))
            def _():
                row_copy(g, zb, core, 0, down).wait_send()

            @pl.when((has_up & (zb < z)) | (up_goes(g) & (zb == z)))
            def _():
                row_copy(g, zb, core, 1, up).wait_send()

            if g in raw:
                @pl.when(jnp.logical_not(is_end & (zb == near)))
                def _():
                    row_copy(g, zb, core, 2, partner).wait_send()
            else:
                row_copy(g, zb, core, 2, partner).wait_send()

    def drain_raw(_):
        for g in raw:
            @pl.when(z == 1)
            def _():
                raw_copy(g, 0, down).wait_send()

            @pl.when(z == zs - 2)
            def _():
                raw_copy(g, 1, up).wait_send()

    def drain_relay(_):
        for o in range(1, cols):
            relay_copy(o).wait_send()
        for k in range(len(parts)):
            near_copy(k, core).wait_send()

    def compute(layer):
        codes_ref = codes_refs[layer]

        def read(t, at):
            return full[layer, t, at, :]

        def write(i, t, at, codes):
            codes_ref[at, pl.ds(t * HDIM, HDIM)] = codes

        tops = peaks_of(read, width, heads)
        note_tops(peaks_ref, layer, tops)
        encode(read, write, tops, width)
        project(codes_ref, pbuf, checked_ref.at[layer], tops)

    for g in raw:
        wait_own(g)

        @pl.when(z == 1)
        def _():
            raw_copy(g, 0, down).start()

        @pl.when(z == zs - 2)
        def _():
            raw_copy(g, 1, up).start()

    for copy in map_copies:
        copy.wait()
    total = cols * heads
    mine = [src_map[mycol * heads + s] for s in range(heads)]
    want = [tgt_map[mycol * heads + t] for t in range(heads)]
    goes = [jnp.int32(0)] * heads
    for p in range(heads, total):
        wanted = tgt_map[p]
        goes = [g + jnp.where(m == wanted, p // heads, 0) for g, m in zip(goes, mine)]
    for o in range(cols):
        to = target_of(o)
        seen, picks = jnp.int32(0), [jnp.int32(0)] * SLOTS
        for s in range(heads):
            hit = goes[s] == to
            picks = [jnp.where(hit & (seen == j), s, q) for j, q in enumerate(picks)]
            seen = seen + jnp.where(hit, 1, 0)
        for j in range(SLOTS):
            table[o * SLOTS + j] = picks[j]
    slot_of = [jnp.int32(0)] * heads
    for c in range(cols):
        seen = jnp.int32(0)
        for s in range(heads):
            held = src_map[c * heads + s]
            for t in range(heads):
                slot_of[t] = jnp.where(want[t] == held, c * SLOTS + seen, slot_of[t])
            hit = want[0] == held
            for t in range(1, heads):
                hit = hit | (want[t] == held)
            seen = jnp.minimum(seen + jnp.where(hit, 1, 0), SLOTS - 1)
    for t in range(heads):
        table[cols * SLOTS + t] = slot_of[t]

    def hand_out_layer(layer):
        for g in range(count):
            if pieces[g][0] == layer:
                if g not in raw:
                    wait_own(g)
                hand_out(g)

    def run(steps):
        for stage, g in steps:
            stage(g)

    def either(ends, mids):
        @pl.when(is_end)
        def _():
            run(ends)

        @pl.when(jnp.logical_not(is_end))
        def _():
            run(mids)

    def finish(layer):
        if layer == 0:
            probe_copy.wait()
        run(of(layer, wait_partner))
        for k, part in enumerate(parts):
            if part[0] == layer:
                @pl.when(is_end)
                def _():
                    near_copy(k, 1 - core).wait_recv()
        compute(layer)

    def of(layer, stage):
        return [(stage, g) for g in range(count) if pieces[g][0] == layer]

    hand_out_layer(0)
    hand_out_layer(1)
    own0, fwd0 = of(0, stage_own), of(0, stage_forward)
    own1, fwd1 = of(1, stage_own), of(1, stage_forward)
    lead = own0[:2]
    for f, o in zip(fwd0, own0[2:] + own1):
        lead += [f, o]
    cut = 2 * len(own0) - 2
    either(own0 + [(relay_out, 0)], lead[:cut])
    for layer in range(2, layers):
        hand_out_layer(layer)
    started = lead[cut:] + fwd0[len(own0) - 2 + len(own1):]
    started += [o for o in own1 if o not in lead]
    later = []
    for layer in range(2, layers):
        later += of(layer, stage_own)
    ahead = len(of(2, stage_own))
    either(
        own1 + fwd0 + [(relay_in, 0)] + later + fwd1,
        started + fwd1[:1] + later[:ahead] + fwd1[1:] + later[ahead:],
    )
    finish(0)
    finish(1)
    for layer in range(2, layers - 1):
        run(of(layer, stage_forward))
        finish(layer)
    *early, end = of(layers - 1, stage_forward)
    *early_in, end_in = of(layers - 1, wait_partner)
    *drains, end_drain = [(drain, g) for g in range(count)]
    either(
        early + [(drain_raw, 0), (drain_relay, 0)] + drains + early_in + [end],
        early + [end, (drain_raw, 0)] + drains + early_in,
    )
    run([end_in, end_drain])


def finish_kernel(
    checked_ref, last_ref, pbuf, peaks_ref, *refs,
):
    done = checked_ref.shape[0]
    codes_refs, refs = refs[:done], refs[done:]
    (
        codes_out, checked_out, peaks_out,
        cbuf, kbuf, tops_ref, codesem, stepsem, checksem, peaksem,
    ) = refs
    heads, width, _ = last_ref.shape
    half = width // 2
    copies = []
    for layer in range(done):
        for i in range(2):
            at = pl.ds(i * half, half)
            copies.append(
                pltpu.make_async_copy(
                    codes_refs[layer].at[at], codes_out.at[layer, at], codesem.at[layer, i]
                )
            )
    copies.append(
        pltpu.make_async_copy(checked_ref, checked_out.at[pl.ds(0, done)], checksem.at[0])
    )
    for copy in copies:
        copy.start()
    tops_ref[...] = peaks_ref[...]

    def step_copy(i):
        at = pl.ds(pl.multiple_of(i * CSTEP, CSTEP), CSTEP)
        return pltpu.make_async_copy(cbuf.at[at], codes_out.at[done, at], stepsem.at[i])

    def read(t, at):
        return last_ref[t, at, :]

    def write(i, t, at, codes):
        cbuf[at, pl.ds(t * HDIM, HDIM)] = codes
        if t == heads - 1:
            step_copy(i).start()

    tops = peaks_of(read, width, heads)
    note_tops(tops_ref, done, tops)
    encode(read, write, tops, width)
    project(cbuf, pbuf, kbuf, tops)
    ends = [
        pltpu.make_async_copy(kbuf, checked_out.at[done], checksem.at[1]),
        pltpu.make_async_copy(tops_ref, peaks_out, peaksem.at[0]),
    ]
    for copy in ends:
        copy.start()
    for copy in copies + ends:
        copy.wait()

    @pl.loop(0, width // CSTEP)
    def _(i):
        step_copy(i).wait()


def finish(gathered, layers, heads, width, span, tokens, dtype):
    done = layers - 1
    anywhere = pl.BlockSpec(memory_space=pl.ANY)
    vmem = pl.BlockSpec(memory_space=pltpu.VMEM)
    dma = pltpu.SemaphoreType.DMA
    codes, checked, peaks = pl.pallas_call(
        finish_kernel,
        out_shape=(
            jax.ShapeDtypeStruct((layers, width, span), dtype),
            jax.ShapeDtypeStruct((layers, tokens, span), dtype),
            jax.ShapeDtypeStruct((layers, heads), jnp.float32),
        ),
        in_specs=[vmem] * (4 + done),
        out_specs=(anywhere,) * 3,
        scratch_shapes=[
            pltpu.VMEM((width, span), dtype),
            pltpu.VMEM((tokens, span), dtype),
            pltpu.VMEM((layers, heads), jnp.float32),
            dma((done, 2)),
            dma((width // CSTEP,)),
            dma((2,)),
            dma((1,)),
        ],
        compiler_params=pltpu.CompilerParams(
            vmem_limit_bytes=2 * width * span + 2 * tokens * span + 2**22
        ),
    )(*[pltpu.with_memory_space_constraint(x, pltpu.VMEM) for x in gathered])
    return codes, peaks, checked


def per_device(train_weight, src_map, tgt_map, probe):
    cols = lax.axis_size("col")
    zs = lax.axis_size("row") // CORES
    layers, rows, span = train_weight.shape
    heads = src_map.shape[0] // cols
    tokens, width = probe.shape
    pieces = piece_list(layers, rows)
    count, done = len(pieces), layers - 1
    dtype = train_weight.dtype
    others = cols - 1
    anywhere = pl.BlockSpec(memory_space=pl.ANY)
    vmem = pl.BlockSpec(memory_space=pltpu.VMEM)
    dma = pltpu.SemaphoreType.DMA
    lane = 2 * HDIM
    results = lane * (heads * (layers * width + done * tokens)) + lane * tokens * (width // HDIM)

    def scratch(raw):
        extra = sum(size for _, size, _ in raw_parts(pieces, raw))
        return extra, lane * (
            done * heads * width
            + layers * rows * (SLOTS * others + heads + SLOTS * cols)
            + extra * (heads + SLOTS * others + SLOTS * cols)
        ) + 2**21

    raw = [g for g in range(count) if pieces[g][0] == 0]
    if results + scratch(raw + [len(raw)])[1] < VMEM:
        raw = raw + [len(raw)]
    extra, grant = scratch(raw)
    maps = [pltpu.with_memory_space_constraint(x, pltpu.HBM) for x in (src_map, tgt_map)]
    gathered = pl.pallas_call(
        functools.partial(gather_kernel, pieces, raw, zs, cols),
        out_shape=(
            pltpu.VMEM((done, tokens, span), dtype),
            pltpu.VMEM((heads, width, HDIM), dtype),
            pltpu.VMEM((tokens, width), dtype),
            pltpu.VMEM((layers, heads), jnp.float32),
        )
        + (pltpu.VMEM((width, span), dtype),) * done,
        in_specs=[pl.BlockSpec(memory_space=pltpu.HBM)] * 2 + [anywhere] * 2,
        out_specs=(vmem,) * (4 + done),
        scratch_shapes=[
            pltpu.VMEM((done, heads, width, HDIM), dtype),
            pltpu.VMEM((layers, others, SLOTS, rows, HDIM), dtype),
            pltpu.VMEM((heads, extra, HDIM), dtype),
            pltpu.VMEM((others, SLOTS, extra, HDIM), dtype),
            pltpu.VMEM((cols * SLOTS, extra, HDIM), dtype),
            pltpu.VMEM((heads, TILE, HDIM), dtype),
            pltpu.SMEM((cols * SLOTS + heads,), jnp.int32),
            pltpu.SMEM(src_map.shape, jnp.int32),
            pltpu.SMEM(tgt_map.shape, jnp.int32),
            dma((2,)),
            dma((count, heads)),
            dma((1,)),
            dma((count, cols)),
            dma((count, cols)),
            dma((count, zs, 3)),
            dma((count, zs * CORES)),
            dma((count, 2)),
            dma((count,)),
            dma((cols,)),
            dma((cols,)),
            dma((2,)),
            dma((2,)),
        ]
        + [pltpu.VMEM((heads, size, HDIM), dtype) for _, _, size in pieces]
        + [pltpu.VMEM((cols * SLOTS, size, HDIM), dtype) for _, _, size in pieces],
        compiler_params=pltpu.CompilerParams(
            collective_id=0, has_side_effects=True, vmem_limit_bytes=grant
        ),
    )(*maps, train_weight, probe)
    return finish(gathered, layers, heads, width, span, tokens, dtype)


def solution(mesh):
    in_specs = (P(None, "row", "col"), P(), P(), P("row", None))
    out_specs = (P(None, None, "col"), P(None, "col"), P(None, "row", "col"))
    return jax.shard_map(
        per_device, mesh=mesh, in_specs=in_specs, out_specs=out_specs, check_vma=False
    )
```

```python
import functools

import jax
import jax.numpy as jnp
from jax import lax
from jax.experimental import pallas as pl
from jax.experimental.pallas import tpu as pltpu
from jax.sharding import PartitionSpec as P

HDIM = 128
CORES = 2
TILE = 16
PSTEP = 128
CSTEP = 512
KSTEP = 4608
NSTEP = 256
SLOTS = 2
VMEM = 63 * 2**20
MESH = pl.DeviceIdType.MESH


def split(rows, shares):
    units, total = rows // TILE, sum(shares)
    cuts = [units * sum(shares[:i]) // total for i in range(len(shares) + 1)]
    return [(a * TILE, (b - a) * TILE) for a, b in zip(cuts, cuts[1:]) if b > a]


def piece_list(layers, rows):
    out = []
    for layer in range(layers):
        if layer == 0:
            shares = (1, 2, 3, 6)
        elif layer == layers - 1:
            shares = (2, 1)
        else:
            shares = (1, 1) if layer == 1 else (1,)
        out.extend((layer, r0, size) for r0, size in split(rows, shares))
    return out


def raw_parts(pieces, raw):
    parts = {}
    for g in raw:
        layer, _, size = pieces[g]
        parts[layer] = parts.get(layer, 0) + size
    out, place = [], 0
    for layer, size in parts.items():
        out.append((layer, size, place))
        place += size
    return out


def peaks_of(read, width, heads):
    def most(i, acc):
        at = pl.ds(pl.multiple_of(i * PSTEP, PSTEP), PSTEP)
        return tuple(
            jnp.maximum(a, jnp.max(jnp.abs(read(t, at)).reshape(-1, TILE, HDIM), axis=0))
            for t, a in enumerate(acc)
        )

    zero = jnp.zeros((TILE, HDIM), jnp.bfloat16)
    best = lax.fori_loop(0, width // PSTEP, most, (zero,) * heads)
    return [
        jnp.max(jnp.max(b.astype(jnp.float32), axis=0, keepdims=True), axis=1, keepdims=True)
        for b in best
    ]


def encode(read, write, tops, width):
    spread = [jnp.broadcast_to(p, (1, HDIM)) for p in tops]
    inverse = [1.0 / ((p + 1e-06) * 0.25) for p in spread]

    @pl.loop(0, width // CSTEP)
    def _(i):
        at = pl.ds(pl.multiple_of(i * CSTEP, CSTEP), CSTEP)
        for t, inv in enumerate(inverse):
            scaled = (read(t, at) * 0.25).astype(jnp.float32) * inv
            write(i, t, at, scaled.astype(jnp.bfloat16))


def project(codes_ref, pbuf, out_ref, tops):
    width, span = codes_ref.shape
    tokens = pbuf.shape[0]
    spread = jnp.concatenate([jnp.broadcast_to(p, (1, HDIM)) for p in tops], axis=1)
    for n0 in range(0, span, NSTEP):
        lanes = pl.ds(n0, NSTEP)

        def step(i, acc):
            at = pl.ds(pl.multiple_of(i * KSTEP, KSTEP), KSTEP)
            return acc + jnp.dot(
                pbuf[:, at], codes_ref[at, lanes], preferred_element_type=jnp.float32
            )

        acc = lax.fori_loop(0, width // KSTEP, step, jnp.zeros((tokens, NSTEP), jnp.float32))
        out_ref[:, lanes] = (acc * spread[:, n0 : n0 + NSTEP]).astype(out_ref.dtype)


def note_tops(peaks_ref, layer, tops):
    here = lax.broadcasted_iota(jnp.int32, peaks_ref.shape, 0) == layer
    lane = lax.broadcasted_iota(jnp.int32, peaks_ref.shape, 1)
    for t, top in enumerate(tops):
        peaks_ref[...] = jnp.where(here & (lane == t), top, peaks_ref[...])


def gather_kernel(
    pieces, raw, zs, cols, src_hbm, tgt_hbm, w_ref, probe_ref,
    checked_ref, last_ref, pbuf, peaks_ref, *refs,
):
    layers, rows, _ = w_ref.shape
    codes_refs, refs = refs[: layers - 1], refs[layers - 1 :]
    (
        full, pack, zown, zpack, zland, guard, table, src_map, tgt_map,
        mapsem, local, probesem, csend, crecv, zsend, zrecv,
        rawsend, rawrecv, rsend, rrecv, psend, precv, *bufs,
    ) = refs
    count = len(pieces)
    own, land = bufs[:count], bufs[count:]
    heads, width, _ = last_ref.shape
    me = lax.axis_index("row")
    mycol = lax.axis_index("col")
    z = me // CORES
    core = me % CORES
    partner = z * CORES + (1 - core)
    down, up = me - CORES, me + CORES
    has_down, has_up = z > 0, z < zs - 1
    low, high = z == 0, z == zs - 1
    is_end = low | high
    near = jnp.where(low, 1, zs - 2)
    parts = raw_parts(pieces, raw)

    def layer_ref(layer):
        return last_ref if layer == layers - 1 else full.at[layer]

    def own_copy(g, head):
        layer, r0, size = pieces[g]
        return pltpu.make_async_copy(
            w_ref.at[layer, pl.ds(r0, size), pl.ds(head * HDIM, HDIM)],
            own[g].at[head],
            local.at[g, head],
        )

    def target_of(o):
        return lax.rem(mycol + cols - o, cols)

    barrier = pltpu.get_barrier_semaphore()
    for o in range(1, cols):
        pl.semaphore_signal(barrier, inc=1, device_id={"col": target_of(o)}, device_id_type=MESH)
    pl.semaphore_signal(barrier, inc=1, device_id={"row": partner}, device_id_type=MESH)

    @pl.when(has_down)
    def _():
        pl.semaphore_signal(barrier, inc=1, device_id={"row": down}, device_id_type=MESH)

    @pl.when(has_up)
    def _():
        pl.semaphore_signal(barrier, inc=1, device_id={"row": up}, device_id_type=MESH)

    for g in raw:
        for head in range(heads):
            own_copy(g, head).start()
    map_copies = [
        pltpu.make_async_copy(src_hbm, src_map, mapsem.at[0]),
        pltpu.make_async_copy(tgt_hbm, tgt_map, mapsem.at[1]),
    ]
    for copy in map_copies:
        copy.start()
    for g in range(len(raw), count):
        for head in range(heads):
            own_copy(g, head).start()
    probe_copy = pltpu.make_async_copy(probe_ref, pbuf, probesem.at[0])
    peaks_ref[...] = jnp.zeros_like(peaks_ref)

    pl.semaphore_wait(barrier, cols + has_down.astype(jnp.int32) + has_up.astype(jnp.int32))

    def raw_copy(g, way, target):
        layer, r0, size = pieces[g]
        place = r0 + sum(n for other, n, _ in parts if other < layer)
        return pltpu.make_async_remote_copy(
            src_ref=own[g],
            dst_ref=zown.at[:, pl.ds(place, size), :],
            send_sem=rawsend.at[g, way],
            recv_sem=rawrecv.at[g],
            device_id={"row": target},
            device_id_type=MESH,
        )

    def col_copy(g, o):
        layer, r0, size = pieces[g]
        return pltpu.make_async_remote_copy(
            src_ref=pack.at[layer, o - 1, :, pl.ds(r0, size), :],
            dst_ref=land[g].at[pl.ds(SLOTS * mycol, SLOTS)],
            send_sem=csend.at[g, o],
            recv_sem=crecv.at[g, o],
            device_id={"col": target_of(o)},
            device_id_type=MESH,
        )

    def relay_copy(o):
        return pltpu.make_async_remote_copy(
            src_ref=zpack.at[o - 1],
            dst_ref=zland.at[pl.ds(SLOTS * mycol, SLOTS)],
            send_sem=rsend.at[o],
            recv_sem=rrecv.at[o],
            device_id={"col": target_of(o)},
            device_id_type=MESH,
        )

    def row_copy(g, zb, cb, way, target):
        layer, r0, size = pieces[g]
        block = zb * CORES + cb
        ref = layer_ref(layer).at[:, pl.ds(pl.multiple_of(block * rows + r0, TILE), size), :]
        return pltpu.make_async_remote_copy(
            src_ref=ref,
            dst_ref=ref,
            send_sem=zsend.at[g, zb, way],
            recv_sem=zrecv.at[g, block],
            device_id={"row": target},
            device_id_type=MESH,
        )

    def near_copy(k, cb):
        layer, size, _ = parts[k]
        start = pl.multiple_of((near * CORES + cb) * rows, TILE)
        ref = layer_ref(layer).at[:, pl.ds(start, size), :]
        return pltpu.make_async_remote_copy(
            src_ref=ref,
            dst_ref=ref,
            send_sem=psend.at[k],
            recv_sem=precv.at[k],
            device_id={"row": partner},
            device_id_type=MESH,
        )

    def most_of(block):
        return jnp.max(block.reshape(-1, TILE, HDIM), axis=0)

    def fill(from_ref, out_ref, land_ref):
        for j in range(SLOTS):
            land_ref[SLOTS * mycol + j] = from_ref[table[j]]

        @pl.loop(1, cols)
        def _(o):
            for j in range(SLOTS):
                out_ref[o - 1, j] = from_ref[table[o * SLOTS + j]]

        @pl.loop(1, cols)
        def _(o):
            for j in range(SLOTS):
                guard[j] = most_of(out_ref[o - 1, j])

    def select(land_ref, place, layer, start, size):
        ref = layer_ref(layer)

        @pl.loop(0, heads)
        def _(t):
            ref[t, pl.ds(start, size), :] = land_ref[table[cols * SLOTS + t], pl.ds(place, size), :]

        @pl.loop(0, heads)
        def _(t):
            guard[t] = most_of(ref[t, pl.ds(start, size), :])

    def hand_out(g):
        layer, r0, size = pieces[g]
        fill(own[g], pack.at[layer, :, :, pl.ds(r0, size), :], land[g])
        for o in range(1, cols):
            col_copy(g, o).start()

    def wait_own(g):
        for head in range(heads):
            own_copy(g, head).wait()

    def down_goes(g):
        return z > 1 if g in raw else has_down

    def up_goes(g):
        return z < zs - 2 if g in raw else has_up

    def stage_own(g):
        layer, r0, size = pieces[g]
        for o in range(1, cols):
            col_copy(g, o).wait_recv()
        select(land[g], 0, layer, pl.multiple_of(me * rows + r0, TILE), size)

        @pl.when(down_goes(g))
        def _():
            row_copy(g, z, core, 0, down).start()

        @pl.when(up_goes(g))
        def _():
            row_copy(g, z, core, 1, up).start()

        row_copy(g, z, core, 2, partner).start()

    def stage_forward(g):
        for h in range(1, zs):
            skips = g in raw and h == 1

            @pl.when((z + h < zs) & (z > 0) if skips else z + h < zs)
            def _():
                row_copy(g, z + h, core, 0, down).wait_recv()

                @pl.when(has_down)
                def _():
                    row_copy(g, z + h, core, 0, down).start()

                row_copy(g, z + h, core, 2, partner).start()

            @pl.when((z - h >= 0) & (z < zs - 1) if skips else z - h >= 0)
            def _():
                row_copy(g, z - h, core, 1, up).wait_recv()

                @pl.when(has_up)
                def _():
                    row_copy(g, z - h, core, 1, up).start()

                row_copy(g, z - h, core, 2, partner).start()

    def relay_out(_):
        for g in raw:
            raw_copy(g, 0, down).wait_recv()
        fill(zown, zpack, zland)
        for o in range(1, cols):
            relay_copy(o).start()

    def relay_in(_):
        for o in range(1, cols):
            relay_copy(o).wait_recv()
        start = pl.multiple_of((near * CORES + core) * rows, TILE)
        for k, (layer, size, place) in enumerate(parts):
            select(zland, place, layer, start, size)
            near_copy(k, core).start()

    def wait_partner(g):
        @pl.loop(0, zs)
        def _(zb):
            if g in raw:
                @pl.when(jnp.logical_not(is_end & (zb == near)))
                def _():
                    row_copy(g, zb, 1 - core, 2, partner).wait_recv()
            else:
                row_copy(g, zb, 1 - core, 2, partner).wait_recv()

    def drain(g):
        for o in range(1, cols):
            col_copy(g, o).wait_send()

        @pl.loop(0, zs)
        def _(zb):
            @pl.when((has_down & (zb > z)) | (down_goes(g) & (zb == z)))
            def _():
                row_copy(g, zb, core, 0, down).wait_send()

            @pl.when((has_up & (zb < z)) | (up_goes(g) & (zb == z)))
            def _():
                row_copy(g, zb, core, 1, up).wait_send()

            if g in raw:
                @pl.when(jnp.logical_not(is_end & (zb == near)))
                def _():
                    row_copy(g, zb, core, 2, partner).wait_send()
            else:
                row_copy(g, zb, core, 2, partner).wait_send()

    def drain_raw(_):
        for g in raw:
            @pl.when(z == 1)
            def _():
                raw_copy(g, 0, down).wait_send()

            @pl.when(z == zs - 2)
            def _():
                raw_copy(g, 1, up).wait_send()

    def drain_relay(_):
        for o in range(1, cols):
            relay_copy(o).wait_send()
        for k in range(len(parts)):
            near_copy(k, core).wait_send()

    def compute(layer):
        codes_ref = codes_refs[layer]

        def read(t, at):
            return full[layer, t, at, :]

        def write(i, t, at, codes):
            codes_ref[at, pl.ds(t * HDIM, HDIM)] = codes

        tops = peaks_of(read, width, heads)
        note_tops(peaks_ref, layer, tops)
        encode(read, write, tops, width)
        project(codes_ref, pbuf, checked_ref.at[layer], tops)

    for g in raw:
        wait_own(g)

        @pl.when(z == 1)
        def _():
            raw_copy(g, 0, down).start()

        @pl.when(z == zs - 2)
        def _():
            raw_copy(g, 1, up).start()

    for copy in map_copies:
        copy.wait()
    total = cols * heads
    mine = [src_map[mycol * heads + s] for s in range(heads)]
    want = [tgt_map[mycol * heads + t] for t in range(heads)]
    goes = [jnp.int32(0)] * heads
    for p in range(heads, total):
        wanted = tgt_map[p]
        goes = [g + jnp.where(m == wanted, p // heads, 0) for g, m in zip(goes, mine)]
    for o in range(cols):
        to = target_of(o)
        seen, picks = jnp.int32(0), [jnp.int32(0)] * SLOTS
        for s in range(heads):
            hit = goes[s] == to
            picks = [jnp.where(hit & (seen == j), s, q) for j, q in enumerate(picks)]
            seen = seen + jnp.where(hit, 1, 0)
        for j in range(SLOTS):
            table[o * SLOTS + j] = picks[j]
    slot_of = [jnp.int32(0)] * heads
    for c in range(cols):
        seen = jnp.int32(0)
        for s in range(heads):
            held = src_map[c * heads + s]
            for t in range(heads):
                slot_of[t] = jnp.where(want[t] == held, c * SLOTS + seen, slot_of[t])
            hit = want[0] == held
            for t in range(1, heads):
                hit = hit | (want[t] == held)
            seen = jnp.minimum(seen + jnp.where(hit, 1, 0), SLOTS - 1)
    for t in range(heads):
        table[cols * SLOTS + t] = slot_of[t]

    def hand_out_layer(layer):
        for g in range(count):
            if pieces[g][0] == layer:
                if g not in raw:
                    wait_own(g)
                hand_out(g)

    def run(steps):
        for stage, g in steps:
            stage(g)

    def either(ends, mids):
        @pl.when(is_end)
        def _():
            run(ends)

        @pl.when(jnp.logical_not(is_end))
        def _():
            run(mids)

    def finish(layer):
        if layer == 0:
            probe_copy.wait()
        run(of(layer, wait_partner))
        for k, part in enumerate(parts):
            if part[0] == layer:
                @pl.when(is_end)
                def _():
                    near_copy(k, 1 - core).wait_recv()
        compute(layer)

    def of(layer, stage):
        return [(stage, g) for g in range(count) if pieces[g][0] == layer]

    hand_out_layer(0)
    probe_copy.start()
    own0, fwd0 = of(0, stage_own), of(0, stage_forward)
    own1, fwd1 = of(1, stage_own), of(1, stage_forward)
    lead = own0[:2]
    for f, o in zip(fwd0, own0[2:] + own1):
        lead += [f, o]
    cut = 2 * len(own0) - 2
    run(own0[:2])
    hand_out_layer(1)
    either(own0[2:] + [(relay_out, 0)], lead[2:cut])
    for layer in range(2, layers):
        hand_out_layer(layer)
    started = lead[cut:] + fwd0[len(own0) - 2 + len(own1):]
    started += [o for o in own1 if o not in lead]
    later = []
    for layer in range(2, layers):
        later += of(layer, stage_own)
    ahead = len(of(2, stage_own))
    either(
        own1 + fwd0 + [(relay_in, 0)] + later + fwd1,
        started + fwd1[:1] + later[:ahead] + fwd1[1:] + later[ahead:],
    )
    finish(0)
    finish(1)
    for layer in range(2, layers - 1):
        run(of(layer, stage_forward))
        finish(layer)
    *early, end = of(layers - 1, stage_forward)
    *early_in, end_in = of(layers - 1, wait_partner)
    *drains, end_drain = [(drain, g) for g in range(count)]
    either(
        early + [(drain_raw, 0), (drain_relay, 0)] + drains + early_in + [end],
        early + [end, (drain_raw, 0)] + drains + early_in,
    )
    run([end_in, end_drain])


def finish_kernel(
    checked_ref, last_ref, pbuf, peaks_ref, *refs,
):
    done = checked_ref.shape[0]
    codes_refs, refs = refs[:done], refs[done:]
    (
        codes_out, checked_out, peaks_out,
        cbuf, kbuf, tops_ref, codesem, stepsem, checksem, peaksem,
    ) = refs
    heads, width, _ = last_ref.shape
    half = width // 2
    copies = []
    for layer in range(done):
        for i in range(2):
            at = pl.ds(i * half, half)
            copies.append(
                pltpu.make_async_copy(
                    codes_refs[layer].at[at], codes_out.at[layer, at], codesem.at[layer, i]
                )
            )
    copies.append(
        pltpu.make_async_copy(checked_ref, checked_out.at[pl.ds(0, done)], checksem.at[0])
    )
    for copy in copies:
        copy.start()
    tops_ref[...] = peaks_ref[...]

    def step_copy(i):
        at = pl.ds(pl.multiple_of(i * CSTEP, CSTEP), CSTEP)
        return pltpu.make_async_copy(cbuf.at[at], codes_out.at[done, at], stepsem.at[i])

    def read(t, at):
        return last_ref[t, at, :]

    def write(i, t, at, codes):
        cbuf[at, pl.ds(t * HDIM, HDIM)] = codes
        if t == heads - 1:
            step_copy(i).start()

    tops = peaks_of(read, width, heads)
    note_tops(tops_ref, done, tops)
    encode(read, write, tops, width)
    project(cbuf, pbuf, kbuf, tops)
    ends = [
        pltpu.make_async_copy(kbuf, checked_out.at[done], checksem.at[1]),
        pltpu.make_async_copy(tops_ref, peaks_out, peaksem.at[0]),
    ]
    for copy in ends:
        copy.start()
    for copy in copies + ends:
        copy.wait()

    @pl.loop(0, width // CSTEP)
    def _(i):
        step_copy(i).wait()


def finish(gathered, layers, heads, width, span, tokens, dtype):
    done = layers - 1
    anywhere = pl.BlockSpec(memory_space=pl.ANY)
    vmem = pl.BlockSpec(memory_space=pltpu.VMEM)
    dma = pltpu.SemaphoreType.DMA
    codes, checked, peaks = pl.pallas_call(
        finish_kernel,
        out_shape=(
            jax.ShapeDtypeStruct((layers, width, span), dtype),
            jax.ShapeDtypeStruct((layers, tokens, span), dtype),
            jax.ShapeDtypeStruct((layers, heads), jnp.float32),
        ),
        in_specs=[vmem] * (4 + done),
        out_specs=(anywhere,) * 3,
        scratch_shapes=[
            pltpu.VMEM((width, span), dtype),
            pltpu.VMEM((tokens, span), dtype),
            pltpu.VMEM((layers, heads), jnp.float32),
            dma((done, 2)),
            dma((width // CSTEP,)),
            dma((2,)),
            dma((1,)),
        ],
        compiler_params=pltpu.CompilerParams(
            vmem_limit_bytes=2 * width * span + 2 * tokens * span + 2**22
        ),
    )(*[pltpu.with_memory_space_constraint(x, pltpu.VMEM) for x in gathered])
    return codes, peaks, checked


def per_device(train_weight, src_map, tgt_map, probe):
    cols = lax.axis_size("col")
    zs = lax.axis_size("row") // CORES
    layers, rows, span = train_weight.shape
    heads = src_map.shape[0] // cols
    tokens, width = probe.shape
    pieces = piece_list(layers, rows)
    count, done = len(pieces), layers - 1
    dtype = train_weight.dtype
    others = cols - 1
    anywhere = pl.BlockSpec(memory_space=pl.ANY)
    vmem = pl.BlockSpec(memory_space=pltpu.VMEM)
    dma = pltpu.SemaphoreType.DMA
    lane = 2 * HDIM
    results = lane * (heads * (layers * width + done * tokens)) + lane * tokens * (width // HDIM)

    def scratch(raw):
        extra = sum(size for _, size, _ in raw_parts(pieces, raw))
        return extra, lane * (
            done * heads * width
            + layers * rows * (SLOTS * others + heads + SLOTS * cols)
            + extra * (heads + SLOTS * others + SLOTS * cols)
        ) + 2**21

    raw = [g for g in range(count) if pieces[g][0] == 0]
    if results + scratch(raw + [len(raw)])[1] < VMEM:
        raw = raw + [len(raw)]
    extra, grant = scratch(raw)
    maps = [pltpu.with_memory_space_constraint(x, pltpu.HBM) for x in (src_map, tgt_map)]
    gathered = pl.pallas_call(
        functools.partial(gather_kernel, pieces, raw, zs, cols),
        out_shape=(
            pltpu.VMEM((done, tokens, span), dtype),
            pltpu.VMEM((heads, width, HDIM), dtype),
            pltpu.VMEM((tokens, width), dtype),
            pltpu.VMEM((layers, heads), jnp.float32),
        )
        + (pltpu.VMEM((width, span), dtype),) * done,
        in_specs=[pl.BlockSpec(memory_space=pltpu.HBM)] * 2 + [anywhere] * 2,
        out_specs=(vmem,) * (4 + done),
        scratch_shapes=[
            pltpu.VMEM((done, heads, width, HDIM), dtype),
            pltpu.VMEM((layers, others, SLOTS, rows, HDIM), dtype),
            pltpu.VMEM((heads, extra, HDIM), dtype),
            pltpu.VMEM((others, SLOTS, extra, HDIM), dtype),
            pltpu.VMEM((cols * SLOTS, extra, HDIM), dtype),
            pltpu.VMEM((heads, TILE, HDIM), dtype),
            pltpu.SMEM((cols * SLOTS + heads,), jnp.int32),
            pltpu.SMEM(src_map.shape, jnp.int32),
            pltpu.SMEM(tgt_map.shape, jnp.int32),
            dma((2,)),
            dma((count, heads)),
            dma((1,)),
            dma((count, cols)),
            dma((count, cols)),
            dma((count, zs, 3)),
            dma((count, zs * CORES)),
            dma((count, 2)),
            dma((count,)),
            dma((cols,)),
            dma((cols,)),
            dma((2,)),
            dma((2,)),
        ]
        + [pltpu.VMEM((heads, size, HDIM), dtype) for _, _, size in pieces]
        + [pltpu.VMEM((cols * SLOTS, size, HDIM), dtype) for _, _, size in pieces],
        compiler_params=pltpu.CompilerParams(
            collective_id=0, has_side_effects=True, vmem_limit_bytes=grant
        ),
    )(*maps, train_weight, probe)
    return finish(gathered, layers, heads, width, span, tokens, dtype)


def solution(mesh):
    in_specs = (P(None, "row", "col"), P(), P(), P("row", None))
    out_specs = (P(None, None, "col"), P(None, "col"), P(None, "row", "col"))
    return jax.shard_map(
        per_device, mesh=mesh, in_specs=in_specs, out_specs=out_specs, check_vma=False
    )
```
